128 devices in a mesh: dp: 1, vp: 128 (over z, y, x, core).
Axes of the slice: x: 4, y: 4, z: 4, core: 2. Of those that a mesh axis runs over, the one named last changes fastest.
Arguments:
- hidden: bfloat16 [2048, 12288], P('dp')
- w_head: bfloat16 [12288, 32768], P(None, 'vp')
- inv_temp: float32 [2048], P('dp')
- target_ids: int32 [2048], P('dp')
Outputs:
- output 1: float32 [2048, 32768], P(('dp', 'vp'))
- output 2: float32 [2048], P('dp')
All inputs are finite; a program needn't handle non-finite values.
Results may differ from the reference program's by a relative error of at most 0.001.
Values are sent between devices in bfloat16 or wider.
A program may use at most 1 GiB of HBM per device.

```python
import math
import jax
import jax.numpy as jnp
from jax import lax

BATCH = 2048
HIDDEN = 12288
VOCAB = 32768
W_ROW_BLOCK = 256


def draw_head(key, direction, profile):
    num_blocks = HIDDEN // W_ROW_BLOCK
    dir_blocks = direction.reshape(num_blocks, W_ROW_BLOCK)

    def one_block(block_args):
        block_idx, dir_rows = block_args
        noise_rows = jax.random.normal(jax.random.fold_in(key, block_idx), (W_ROW_BLOCK, VOCAB), jnp.float32)
        head_rows = (noise_rows + dir_rows[:, None] * profile[None, :]) * (HIDDEN ** -0.5)
        return head_rows.astype(jnp.bfloat16)

    blocks = lax.map(one_block, (jnp.arange(num_blocks), dir_blocks))
    return blocks.reshape(HIDDEN, VOCAB)


def setup_inputs(seed: int = 0, part: int = 0) -> dict:
    base_key = jax.random.key(seed)
    shared_key = jax.random.fold_in(base_key, 1)
    part_key = jax.random.fold_in(jax.random.fold_in(base_key, 2), part)
    key_dir, key_head = jax.random.split(shared_key)
    key_hid, key_gain, key_temp, key_ids = jax.random.split(part_key, 4)
    direction = jax.random.normal(key_dir, (HIDDEN,), jnp.float32)
    vocab_pos = jnp.arange(VOCAB, dtype=jnp.float32) / VOCAB
    profile = 1.5 * jnp.exp(-8.0 * vocab_pos)
    w_head = draw_head(key_head, direction, profile)
    row_gain = 2.0 + 0.5 * jax.random.normal(key_gain, (BATCH, 1), jnp.float32)
    hidden = jax.random.normal(key_hid, (BATCH, HIDDEN), jnp.float32) + row_gain * direction[None, :] * (HIDDEN ** -0.5)
    row_pos = jnp.arange(BATCH)
    log_temp = jax.random.uniform(key_temp, (BATCH,), jnp.float32, minval=math.log(0.5), maxval=math.log(32.0))
    inv_temp = jnp.where(row_pos == 0, 32.0, jnp.exp(log_temp))
    target_ids = jax.random.randint(key_ids, (BATCH,), 0, VOCAB, dtype=jnp.int32)
    target_ids = jnp.where(row_pos == 1, VOCAB - 1, target_ids)
    return {"hidden": hidden.astype(jnp.bfloat16), "w_head": w_head, "inv_temp": inv_temp, "target_ids": target_ids}


def reference(hidden, w_head, inv_temp, target_ids):
    logits = jnp.dot(hidden, w_head, preferred_element_type=jnp.float32)
    scaled = logits * inv_temp[:, None]
    row_max = jnp.max(scaled, axis=1, keepdims=True)
    exp_vals = jnp.exp(scaled - row_max)
    probabilities = exp_vals / jnp.sum(exp_vals, axis=1, keepdims=True)
    cdf_table = jnp.cumsum(probabilities, axis=1)
    cdf_at_target = jnp.take_along_axis(cdf_table, target_ids[:, None], axis=1)[:, 0]
    return cdf_table, cdf_at_target
```

```python
import functools

import jax
import jax.numpy as jnp
from jax import lax
from jax.experimental import pallas as pl
from jax.experimental.pallas import tpu as pltpu
from jax.sharding import PartitionSpec as P

MESH = pl.DeviceIdType.MESH
STRIDE = 37
SLOTS = 3


def split3(x):
    hi = x.astype(jnp.bfloat16)
    rest = x - hi.astype(jnp.float32)
    mid = rest.astype(jnp.bfloat16)
    lo = (rest - mid.astype(jnp.float32)).astype(jnp.bfloat16)
    return hi, mid, lo


def exact_dot(x, ones_mask):
    hi, mid, lo = split3(x)
    dot = functools.partial(jnp.dot, preferred_element_type=jnp.float32)
    return dot(lo, ones_mask) + dot(mid, ones_mask) + dot(hi, ones_mask)


def exchange_kernel(
    n, rows, group,
    hidden, w, temp, target,
    cum_out, scale_out, off_out, tgt_out,
    w_buf, h_buf, send, recv, cum, tsend, trecv,
    w_sem, h_sem, send_sem, recv_sem, out_sem, tsend_sem, trecv_sem,
):
    me = lax.axis_index("vp")
    cols = w.shape[1]
    steps = n // group
    bits = n.bit_length() - 1
    my_bits = [lax.rem(lax.div(me, 1 << i), 2) for i in range(bits)]

    def peer(k):
        p = lax.rem(k * STRIDE, n)
        return sum(lax.rem(my_bits[i] + lax.div(p, 1 << i), 2) * (1 << i) for i in range(bits))

    def h_copy(slot, j, d):
        return pltpu.make_async_copy(
            hidden.at[pl.ds(pl.multiple_of(d * rows, rows), rows)],
            h_buf.at[slot, pl.ds(j * rows, rows)],
            h_sem.at[slot],
        )

    def fetch(step):
        slot = lax.rem(step, SLOTS)
        for j in range(group):
            h_copy(slot, j, peer(step * group + j + 1)).start()

    def fetched(slot):
        pltpu.make_async_copy(h_buf.at[slot], h_buf.at[slot], h_sem.at[slot]).wait()

    w_parts = 4
    part = w.shape[0] // w_parts
    fetch(0)
    for i in range(w_parts):
        at = pl.ds(i * part, part)
        pltpu.make_async_copy(w.at[at], w_buf.at[at], w_sem).start()
    for s in range(1, SLOTS - 1):
        fetch(s)

    barrier = pltpu.get_barrier_semaphore()

    def greet(k, carry):
        pl.semaphore_signal(barrier, inc=1, device_id={"vp": peer(k)}, device_id_type=MESH)
        return carry

    lax.fori_loop(1, n, greet, 0)

    def block_copy(step, j):
        d = peer(step * group + j + 1)
        return pltpu.make_async_remote_copy(
            src_ref=send.at[step * group + j],
            dst_ref=recv.at[me],
            send_sem=send_sem,
            recv_sem=recv_sem.at[step],
            device_id={"vp": d},
            device_id_type=MESH,
        )

    def multiply(step):
        slot = lax.rem(step, SLOTS)
        z = jnp.dot(h_buf[slot], w_buf[...], preferred_element_type=jnp.float32)
        send[pl.ds(step * group, group)] = z.reshape(group, rows, cols)

    pltpu.make_async_copy(w_buf, w_buf, w_sem).wait()

    def matmul_step(step, carry):
        fetched(lax.rem(step, SLOTS))

        @pl.when(step == 1)
        def _():
            pl.semaphore_wait(barrier, n - 1)

        @pl.when(step >= 1)
        def _():
            for j in range(group):
                block_copy(step - 1, j).start()

        @pl.when(step + SLOTS - 1 < steps)
        def _():
            fetch(step + SLOTS - 1)

        multiply(step)
        return carry

    lax.fori_loop(0, steps, matmul_step, 0)

    per = 128 // rows
    lane = lax.broadcasted_iota(jnp.int32, (rows, 128), 1)
    row = lax.broadcasted_iota(jnp.int32, (rows, 128), 0)
    own_lane = lane == lax.rem(me, per) * rows + row
    own_at = pl.ds(lax.div(me, per), 1)
    t_col = jnp.sum(jnp.where(own_lane, temp[own_at, :], 0.0), axis=1, keepdims=True)
    g_col = jnp.sum(jnp.where(own_lane, target[own_at, :], 0), axis=1, keepdims=True)
    upto = (
        lax.broadcasted_iota(jnp.int32, (cols, cols), 0) <= lax.broadcasted_iota(jnp.int32, (cols, cols), 1)
    ).astype(jnp.float32).astype(jnp.bfloat16)
    col = lax.broadcasted_iota(jnp.int32, (rows, cols), 1)

    for j in range(group - 1):
        block_copy(steps - 1, j).start()
    recv[me] = send[n - 1]

    def take(step, carry):
        m_all, s_all, t_acc = carry

        @pl.when(step < steps - 1)
        def _():
            whole = recv.at[pl.ds(0, group)]
            pltpu.make_async_copy(whole, whole, recv_sem.at[step]).wait()

        @pl.when(step == steps - 1)
        def _():
            whole = recv.at[pl.ds(0, group - 1)]
            pltpu.make_async_copy(whole, whole, recv_sem.at[step]).wait()

        source = [peer(step * group + j + 1) for j in range(group)]
        z = [recv[s] * t_col for s in source]
        m = [jnp.max(v, axis=1, keepdims=True) for v in z]
        e = jnp.concatenate([jnp.exp(v - u) for v, u in zip(z, m)], axis=0)
        c = exact_dot(e, upto)
        for j, s in enumerate(source):
            c_j = c[j * rows : (j + 1) * rows]
            cum[s] = c_j
            here = lane == s
            m_all = jnp.where(here, m[j], m_all)
            s_all = jnp.where(here, c_j[:, cols - 1 :], s_all)
            t_acc = t_acc + jnp.where(col == g_col - s * cols, c_j, 0.0)
            pltpu.make_async_copy(cum.at[s], cum_out.at[s], out_sem).start()
        return m_all, s_all, t_acc

    zero = jnp.zeros((rows, 128), jnp.float32)
    m_all, s_all, t_acc = lax.fori_loop(0, steps, take, (zero, zero, jnp.zeros((rows, cols), jnp.float32)))

    top = jnp.max(m_all, axis=1, keepdims=True)
    weight = jnp.exp(m_all - top)
    mass = s_all * weight
    total = jnp.sum(mass, axis=1, keepdims=True)
    before = (
        lax.broadcasted_iota(jnp.int32, (n, n), 0) < lax.broadcasted_iota(jnp.int32, (n, n), 1)
    ).astype(jnp.float32).astype(jnp.bfloat16)
    scale = weight / total
    off = exact_dot(mass / total, before)
    t_cum = jnp.sum(t_acc, axis=1, keepdims=True)
    t_here = lane == lax.div(g_col, cols)
    t_scale = jnp.sum(jnp.where(t_here, scale, 0.0), axis=1, keepdims=True)
    t_off = jnp.sum(jnp.where(t_here, off, 0.0), axis=1, keepdims=True)
    t_val = t_cum * t_scale + t_off
    t_row = jnp.sum(jnp.where(own_lane, t_val, 0.0), axis=0, keepdims=True)
    tsend[...] = jnp.broadcast_to(t_row, tsend.shape)
    scale_out[...] = scale
    off_out[...] = off
    trecv[pl.ds(me, 1), :] = t_row
    pltpu.make_async_copy(cum, cum, out_sem).wait()

    def tell(k, carry):
        pltpu.make_async_remote_copy(
            src_ref=tsend.at[pl.ds(0, 1)],
            dst_ref=trecv.at[pl.ds(me, 1)],
            send_sem=tsend_sem,
            recv_sem=trecv_sem,
            device_id={"vp": peer(k)},
            device_id_type=MESH,
        ).start()
        return carry

    lax.fori_loop(1, n, tell, 0)
    others = trecv.at[pl.ds(0, n - 1)]
    pltpu.make_async_copy(others, others, trecv_sem).wait()
    tgt_out[...] = jnp.sum(trecv[...].reshape(n // per, per, 128), axis=1)
    pltpu.make_async_copy(others, others, tsend_sem).wait()
    sent = send.at[pl.ds(0, n - 1)]
    pltpu.make_async_copy(sent, sent, send_sem).wait()


def finish_kernel(span, cum, scale, off, tgt, table, tgt_out):
    shift = lax.rem(128 - pl.program_id(0) * span, 128)
    sc = pltpu.roll(scale[...], shift, 1)
    of = pltpu.roll(off[...], shift, 1)
    cols = cum.shape[2]
    for i in range(span):
        table[:, i * cols : (i + 1) * cols] = cum[i] * sc[:, i : i + 1] + of[:, i : i + 1]
    tgt_out[...] = tgt[...]


def solution(mesh):
    n = mesh.shape["vp"]

    def local_step(hidden, w_local, inv_temp, target_ids):
        batch, depth = hidden.shape
        cols = w_local.shape[1]
        rows = batch // n
        group = 8
        f32 = jnp.float32
        vmem = pl.BlockSpec(memory_space=pltpu.VMEM)
        hbm = pl.BlockSpec(memory_space=pl.ANY)
        cum, scale, off, tgt = pl.pallas_call(
            functools.partial(exchange_kernel, n, rows, group),
            out_shape=(
                jax.ShapeDtypeStruct((n, rows, cols), f32),
                jax.ShapeDtypeStruct((rows, 128), f32),
                jax.ShapeDtypeStruct((rows, 128), f32),
                jax.ShapeDtypeStruct((batch // 128, 128), f32),
            ),
            in_specs=[hbm, hbm, vmem, vmem],
            out_specs=(hbm, vmem, vmem, vmem),
            scratch_shapes=[
                pltpu.VMEM((depth, cols), jnp.bfloat16),
                pltpu.VMEM((SLOTS, group * rows, depth), jnp.bfloat16),
                pltpu.VMEM((n, rows, cols), f32),
                pltpu.VMEM((n, rows, cols), f32),
                pltpu.VMEM((n, rows, cols), f32),
                pltpu.VMEM((8, 128), f32),
                pltpu.VMEM((n, 128), f32),
                pltpu.SemaphoreType.DMA,
                pltpu.SemaphoreType.DMA((SLOTS,)),
                pltpu.SemaphoreType.DMA,
                pltpu.SemaphoreType.DMA((n // group,)),
                pltpu.SemaphoreType.DMA,
                pltpu.SemaphoreType.DMA,
                pltpu.SemaphoreType.DMA,
            ],
            compiler_params=pltpu.CompilerParams(
                collective_id=0, has_side_effects=True, vmem_limit_bytes=48 * 1024 * 1024
            ),
            name="exchange",
        )(hidden, w_local, inv_temp.reshape(-1, 128), target_ids.reshape(-1, 128))
        span = 16
        whole = lambda i: (0, 0)
        table, at_target = pl.pallas_call(
            functools.partial(finish_kernel, span),
            out_shape=(
                jax.ShapeDtypeStruct((rows, n * cols), f32),
                jax.ShapeDtypeStruct((batch // 128, 128), f32),
            ),
            grid=(n // span,),
            in_specs=[
                pl.BlockSpec((span, rows, cols), lambda i: (i, 0, 0)),
                pl.BlockSpec((rows, 128), whole),
                pl.BlockSpec((rows, 128), whole),
                pl.BlockSpec((batch // 128, 128), whole),
            ],
            out_specs=(
                pl.BlockSpec((rows, span * cols), lambda i: (0, i)),
                pl.BlockSpec((batch // 128, 128), whole),
            ),
            name="finish",
        )(cum, scale, off, tgt)
        return table, at_target.reshape(-1)

    return jax.shard_map(
        local_step,
        mesh=mesh,
        in_specs=(P("dp", None), P(None, "vp"), P("dp"), P("dp")),
        out_specs=(P(("dp", "vp"), None), P("dp")),
        check_vma=False,
    )
```

```python
import functools

import jax
import jax.numpy as jnp
from jax import lax
from jax.experimental import pallas as pl
from jax.experimental.pallas import tpu as pltpu
from jax.sharding import PartitionSpec as P

MESH = pl.DeviceIdType.MESH
SLOTS = 3
FINE = ((1, 3, 5), (2, 4, 6), (0,))
COARSE = (3, 4, 5, 6)


def split3(x):
    hi = x.astype(jnp.bfloat16)
    rest = x - hi.astype(jnp.float32)
    mid = rest.astype(jnp.bfloat16)
    lo = (rest - mid.astype(jnp.float32)).astype(jnp.bfloat16)
    return hi, mid, lo


def exact_dot(x, ones_mask):
    hi, mid, lo = split3(x)
    dot = functools.partial(jnp.dot, preferred_element_type=jnp.float32)
    return dot(lo, ones_mask) + dot(mid, ones_mask) + dot(hi, ones_mask)


def partners(me, step, steps):
    turned = steps - 1 - step
    bits = []
    for i in range(7):
        bit = lax.rem(lax.div(me, 1 << i), 2)
        if i in COARSE:
            bit = lax.rem(bit + lax.div(turned, 1 << COARSE.index(i)), 2)
        bits.append(bit)
    base = sum(b * (1 << i) for i, b in enumerate(bits))
    move = [sum((1 - 2 * bits[i]) * (1 << i) for i in fine) for fine in FINE]
    return [base + sum(m for t, m in enumerate(move) if (7 - j) >> t & 1) for j in range(8)]


def exchange_kernel(
    n, rows, group,
    hidden, w, temp_hbm, target_hbm,
    table, tgt_out,
    w_buf, h_buf, send, recv, cum, temp, target, tsend, trecv,
    w_sem, h_sem, send_sem, recv_sem, small_sem, tsend_sem, trecv_sem,
):
    me = lax.axis_index("vp")
    cols = w.shape[1]
    steps = n // group

    def fetch(step):
        slot = lax.rem(step, SLOTS)
        for j, d in enumerate(partners(me, step, steps)):
            pltpu.make_async_copy(
                hidden.at[pl.ds(pl.multiple_of(d * rows, rows), rows)],
                h_buf.at[slot, pl.ds(j * rows, rows)],
                h_sem.at[slot],
            ).start()

    fetch(0)
    part = w.shape[0] // 4
    for i in range(4):
        at = pl.ds(i * part, part)
        pltpu.make_async_copy(w.at[at], w_buf.at[at], w_sem).start()
    barrier = pltpu.get_barrier_semaphore()

    def greet(step, carry):
        for j, d in enumerate(partners(me, step, steps)):
            if j < group - 1:
                pl.semaphore_signal(barrier, inc=1, device_id={"vp": d}, device_id_type=MESH)
            else:

                @pl.when(step < steps - 1)
                def _():
                    pl.semaphore_signal(barrier, inc=1, device_id={"vp": d}, device_id_type=MESH)

        return carry

    lax.fori_loop(0, steps, greet, 0)
    for s in range(1, SLOTS - 1):
        fetch(s)
    pltpu.make_async_copy(temp_hbm, temp, small_sem).start()
    pltpu.make_async_copy(target_hbm, target, small_sem).start()

    def send_blocks(step, count):
        for j, d in enumerate(partners(me, step, steps)[:count]):
            pltpu.make_async_remote_copy(
                src_ref=send.at[step * group + j],
                dst_ref=recv.at[me],
                send_sem=send_sem,
                recv_sem=recv_sem.at[step],
                device_id={"vp": d},
                device_id_type=MESH,
            ).start()

    pltpu.make_async_copy(w_buf, w_buf, w_sem).wait()

    def matmul_step(step, carry):
        slot = lax.rem(step, SLOTS)
        pltpu.make_async_copy(h_buf.at[slot], h_buf.at[slot], h_sem.at[slot]).wait()

        @pl.when(step == 1)
        def _():
            pl.semaphore_wait(barrier, n - 1)

        @pl.when(step >= 1)
        def _():
            send_blocks(step - 1, group)

        @pl.when(step + SLOTS - 1 < steps)
        def _():
            fetch(step + SLOTS - 1)

        z = jnp.dot(h_buf[slot], w_buf[...], preferred_element_type=jnp.float32)
        send[pl.ds(step * group, group)] = z.reshape(group, rows, cols)
        return carry

    lax.fori_loop(0, steps, matmul_step, 0)
    pltpu.make_async_copy(temp, temp, small_sem).wait()
    pltpu.make_async_copy(target, target, small_sem).wait()

    per = 128 // rows
    lane = lax.broadcasted_iota(jnp.int32, (rows, 128), 1)
    row = lax.broadcasted_iota(jnp.int32, (rows, 128), 0)
    own_lane = lane == lax.rem(me, per) * rows + row
    own_at = pl.ds(lax.div(me, per), 1)
    t_col = jnp.sum(jnp.where(own_lane, temp[own_at, :], 0.0), axis=1, keepdims=True)
    g_col = jnp.sum(jnp.where(own_lane, target[own_at, :], 0), axis=1, keepdims=True)
    upto = (
        lax.broadcasted_iota(jnp.int32, (cols, cols), 0) <= lax.broadcasted_iota(jnp.int32, (cols, cols), 1)
    ).astype(jnp.float32).astype(jnp.bfloat16)
    col = lax.broadcasted_iota(jnp.int32, (rows, cols), 1)

    send_blocks(steps - 1, group - 1)
    recv[me] = send[n - 1]

    def take(step, carry):
        m_all, s_all, t_acc = carry

        @pl.when(step < steps - 1)
        def _():
            whole = recv.at[pl.ds(0, group)]
            pltpu.make_async_copy(whole, whole, recv_sem.at[step]).wait()

        @pl.when(step == steps - 1)
        def _():
            whole = recv.at[pl.ds(0, group - 1)]
            pltpu.make_async_copy(whole, whole, recv_sem.at[step]).wait()

        source = partners(me, step, steps)
        z = [recv[s] * t_col for s in source]
        m = [jnp.max(v, axis=1, keepdims=True) for v in z]
        e = jnp.concatenate([jnp.exp(v - u) for v, u in zip(z, m)], axis=0)
        c = exact_dot(e, upto)
        for j, s in enumerate(source):
            c_j = c[j * rows : (j + 1) * rows]
            cum[s] = c_j
            here = lane == s
            m_all = jnp.where(here, m[j], m_all)
            s_all = jnp.where(here, c_j[:, cols - 1 :], s_all)
            t_acc = t_acc + jnp.where(col == g_col - s * cols, c_j, 0.0)
        return m_all, s_all, t_acc

    zero = jnp.zeros((rows, 128), jnp.float32)
    m_all, s_all, t_acc = lax.fori_loop(0, steps, take, (zero, zero, jnp.zeros((rows, cols), jnp.float32)))

    top = jnp.max(m_all, axis=1, keepdims=True)
    weight = jnp.exp(m_all - top)
    mass = s_all * weight
    total = jnp.sum(mass, axis=1, keepdims=True)
    before = (
        lax.broadcasted_iota(jnp.int32, (n, n), 0) < lax.broadcasted_iota(jnp.int32, (n, n), 1)
    ).astype(jnp.float32).astype(jnp.bfloat16)
    scale = weight / total
    off = exact_dot(mass / total, before)
    t_cum = jnp.sum(t_acc, axis=1, keepdims=True)
    t_here = lane == lax.div(g_col, cols)
    t_scale = jnp.sum(jnp.where(t_here, scale, 0.0), axis=1, keepdims=True)
    t_off = jnp.sum(jnp.where(t_here, off, 0.0), axis=1, keepdims=True)
    t_val = t_cum * t_scale + t_off
    t_row = jnp.sum(jnp.where(own_lane, t_val, 0.0), axis=0, keepdims=True)
    tsend[...] = jnp.broadcast_to(t_row, tsend.shape)
    trecv[pl.ds(me, 1), :] = t_row
    sent = send.at[pl.ds(0, n - 1)]
    pltpu.make_async_copy(sent, sent, send_sem).wait()

    def tell_one(d):
        pltpu.make_async_remote_copy(
            src_ref=tsend.at[pl.ds(0, 1)],
            dst_ref=trecv.at[pl.ds(me, 1)],
            send_sem=tsend_sem,
            recv_sem=trecv_sem,
            device_id={"vp": d},
            device_id_type=MESH,
        ).start()

    def tell(step, carry):
        for j, d in enumerate(partners(me, step, steps)):
            if j < group - 1:
                tell_one(d)
            else:
                pl.when(step < steps - 1)(functools.partial(tell_one, d))
        return carry

    lax.fori_loop(0, steps, tell, 0)
    for s in range(n):
        table[:, s * cols : (s + 1) * cols] = cum[s] * scale[:, s : s + 1] + off[:, s : s + 1]
    others = trecv.at[pl.ds(0, n - 1)]
    pltpu.make_async_copy(others, others, trecv_sem).wait()
    tgt_out[...] = jnp.sum(trecv[...].reshape(n // per, per, 128), axis=1)
    pltpu.make_async_copy(others, others, tsend_sem).wait()


def solution(mesh):
    n = mesh.shape["vp"]

    def local_step(hidden, w_local, inv_temp, target_ids):
        batch, depth = hidden.shape
        cols = w_local.shape[1]
        rows = batch // n
        group = 8
        f32 = jnp.float32
        vmem = pl.BlockSpec(memory_space=pltpu.VMEM)
        hbm = pl.BlockSpec(memory_space=pltpu.HBM)
        small = (batch // 128, 128)
        table, at_target = pl.pallas_call(
            functools.partial(exchange_kernel, n, rows, group),
            out_shape=(
                jax.ShapeDtypeStruct((rows, n * cols), f32),
                jax.ShapeDtypeStruct(small, f32),
            ),
            in_specs=[hbm] * 4,
            out_specs=(vmem, vmem),
            scratch_shapes=[
                pltpu.VMEM((depth, cols), jnp.bfloat16),
                pltpu.VMEM((SLOTS, group * rows, depth), jnp.bfloat16),
                pltpu.VMEM((n, rows, cols), f32),
                pltpu.VMEM((n, rows, cols), f32),
                pltpu.VMEM((n, rows, cols), f32),
                pltpu.VMEM(small, f32),
                pltpu.VMEM(small, jnp.int32),
                pltpu.VMEM((8, 128), f32),
                pltpu.VMEM((n, 128), f32),
                pltpu.SemaphoreType.DMA,
                pltpu.SemaphoreType.DMA((SLOTS,)),
                pltpu.SemaphoreType.DMA,
                pltpu.SemaphoreType.DMA((n // group,)),
                pltpu.SemaphoreType.DMA,
                pltpu.SemaphoreType.DMA,
                pltpu.SemaphoreType.DMA,
            ],
            compiler_params=pltpu.CompilerParams(
                collective_id=0, has_side_effects=True, vmem_limit_bytes=48 * 1024 * 1024
            ),
            name="exchange",
        )(hidden, w_local, inv_temp.reshape(small), target_ids.reshape(small))
        return table, at_target.reshape(-1)

    return jax.shard_map(
        local_step,
        mesh=mesh,
        in_specs=(P("dp", None), P(None, "vp"), P("dp"), P("dp")),
        out_specs=(P(("dp", "vp"), None), P("dp")),
        check_vma=False,
    )
```

```python
import functools

import jax
import jax.numpy as jnp
from jax import lax
from jax.experimental import pallas as pl
from jax.experimental.pallas import tpu as pltpu
from jax.sharding import PartitionSpec as P

MESH = pl.DeviceIdType.MESH
SLOTS = 3
FINE = ((1, 4, 6), (3, 6, 2), (5, 2, 4))
COARSE = (0, 2, 4, 6)
PACE = (1, 1)


def split3(x):
    hi = x.astype(jnp.bfloat16)
    rest = x - hi.astype(jnp.float32)
    mid = rest.astype(jnp.bfloat16)
    lo = (rest - mid.astype(jnp.float32)).astype(jnp.bfloat16)
    return hi, mid, lo


def exact_dot(x, ones_mask):
    hi, mid, lo = split3(x)
    dot = functools.partial(jnp.dot, preferred_element_type=jnp.float32)
    return dot(lo, ones_mask) + dot(mid, ones_mask) + dot(hi, ones_mask)


def partners(me, step, steps, sign=1):
    turned = steps - 1 - step
    coarse = [lax.rem(lax.div(turned, 1 << COARSE.index(i)), 2) if i in COARSE else 0 for i in range(7)]
    flipped = lambda bit, flip: 1 - bit if flip else bit
    core = lax.rem(me, 2)
    own = [lax.rem(lax.div(me, 2 * 4**a), 4) for a in range(3)]
    known = {}
    group = []
    for j in range(8):
        fine = [sum(i in f for t, f in enumerate(FINE) if (7 - j) >> t & 1) % 2 for i in range(7)]
        if (0, fine[0]) not in known:
            known[0, fine[0]] = lax.rem(core + flipped(coarse[0], fine[0]), 2)
        parts = [known[0, fine[0]]]
        for a in range(3):
            low, high = fine[2 * a + 1], fine[2 * a + 2]
            if (a + 1, low, high) not in known:
                offset = flipped(coarse[2 * a + 1], low) + 2 * flipped(coarse[2 * a + 2], high)
                moved = own[a] + offset if sign > 0 else own[a] + 4 - offset
                known[a + 1, low, high] = lax.rem(moved, 4) * (2 * 4**a)
            parts.append(known[a + 1, low, high])
        group.append(sum(parts))
    return group


def exchange_kernel(
    n, rows, group,
    hidden, w, temp_hbm, target_hbm,
    table, tgt_out,
    w_buf, h_buf, send, recv, cum, temp, target, tsend, trecv,
    w_sem, h_sem, send_sem, recv_sem, small_sem, tsend_sem, trecv_sem,
):
    me = lax.axis_index("vp")
    cols = w.shape[1]
    steps = n // group

    def fetch(step):
        slot = lax.rem(step, SLOTS)
        for j, d in enumerate(partners(me, step, steps)):
            pltpu.make_async_copy(
                hidden.at[pl.ds(pl.multiple_of(d * rows, rows), rows)],
                h_buf.at[slot, pl.ds(j * rows, rows)],
                h_sem.at[slot],
            ).start()

    barrier = pltpu.get_barrier_semaphore()

    def greet(step, carry):
        for j, d in enumerate(partners(me, step, steps)):
            if j < group - 1:
                pl.semaphore_signal(barrier, inc=1, device_id={"vp": d}, device_id_type=MESH)
            else:

                @pl.when(step < steps - 1)
                def _():
                    pl.semaphore_signal(barrier, inc=1, device_id={"vp": d}, device_id_type=MESH)

        return carry

    lax.fori_loop(0, steps, greet, 0)
    fetch(0)
    part = w.shape[0] // 4
    for i in range(4):
        at = pl.ds(i * part, part)
        pltpu.make_async_copy(w.at[at], w_buf.at[at], w_sem).start()
    for s in range(1, SLOTS - 1):
        fetch(s)
    pltpu.make_async_copy(temp_hbm, temp, small_sem).start()
    pltpu.make_async_copy(target_hbm, target, small_sem).start()

    def send_blocks(step, count):
        for j, d in enumerate(partners(me, step, steps)[:count]):
            pltpu.make_async_remote_copy(
                src_ref=send.at[step * group + j],
                dst_ref=recv.at[me],
                send_sem=send_sem,
                recv_sem=recv_sem.at[step],
                device_id={"vp": d},
                device_id_type=MESH,
            ).start()

    pltpu.make_async_copy(w_buf, w_buf, w_sem).wait()

    def due(step):
        return lax.div(jnp.maximum(step, 0) * PACE[0], PACE[1])

    def matmul_step(step, carry):
        slot = lax.rem(step, SLOTS)
        pltpu.make_async_copy(h_buf.at[slot], h_buf.at[slot], h_sem.at[slot]).wait()

        @pl.when(step == 1)
        def _():
            pl.semaphore_wait(barrier, n - 1)

        @pl.when(due(step) > due(step - 1))
        def _():
            send_blocks(due(step) - 1, group)

        @pl.when(step + SLOTS - 1 < steps)
        def _():
            fetch(step + SLOTS - 1)

        z = jnp.dot(h_buf[slot], w_buf[...], preferred_element_type=jnp.float32)
        send[pl.ds(step * group, group)] = z.reshape(group, rows, cols)
        return carry

    lax.fori_loop(0, steps, matmul_step, 0)
    pltpu.make_async_copy(temp, temp, small_sem).wait()
    pltpu.make_async_copy(target, target, small_sem).wait()

    per = 128 // rows
    lane = lax.broadcasted_iota(jnp.int32, (rows, 128), 1)
    row = lax.broadcasted_iota(jnp.int32, (rows, 128), 0)
    own_lane = lane == lax.rem(me, per) * rows + row
    own_at = pl.ds(lax.div(me, per), 1)
    t_col = jnp.sum(jnp.where(own_lane, temp[own_at, :], 0.0), axis=1, keepdims=True)
    g_col = jnp.sum(jnp.where(own_lane, target[own_at, :], 0), axis=1, keepdims=True)
    upto = (
        lax.broadcasted_iota(jnp.int32, (cols, cols), 0) <= lax.broadcasted_iota(jnp.int32, (cols, cols), 1)
    ).astype(jnp.float32).astype(jnp.bfloat16)
    col = lax.broadcasted_iota(jnp.int32, (rows, cols), 1)

    for step in range((steps - 1) * PACE[0] // PACE[1], steps):
        send_blocks(step, group if step < steps - 1 else group - 1)
    recv[me] = send[n - 1]

    def take(step, carry):
        m_all, s_all, t_acc = carry

        @pl.when(step < steps - 1)
        def _():
            whole = recv.at[pl.ds(0, group)]
            pltpu.make_async_copy(whole, whole, recv_sem.at[step]).wait()

        @pl.when(step == steps - 1)
        def _():
            whole = recv.at[pl.ds(0, group - 1)]
            pltpu.make_async_copy(whole, whole, recv_sem.at[step]).wait()

        source = partners(me, step, steps, -1)
        z = [recv[s] * t_col for s in source]
        m = [jnp.max(v, axis=1, keepdims=True) for v in z]
        e = jnp.concatenate([jnp.exp(v - u) for v, u in zip(z, m)], axis=0)
        c = exact_dot(e, upto)
        for j, s in enumerate(source):
            c_j = c[j * rows : (j + 1) * rows]
            cum[s] = c_j
            here = lane == s
            m_all = jnp.where(here, m[j], m_all)
            s_all = jnp.where(here, c_j[:, cols - 1 :], s_all)
            t_acc = t_acc + jnp.where(col == g_col - s * cols, c_j, 0.0)
        return m_all, s_all, t_acc

    zero = jnp.zeros((rows, 128), jnp.float32)
    m_all, s_all, t_acc = lax.fori_loop(0, steps, take, (zero, zero, jnp.zeros((rows, cols), jnp.float32)))

    top = jnp.max(m_all, axis=1, keepdims=True)
    weight = jnp.exp(m_all - top)
    mass = s_all * weight
    total = jnp.sum(mass, axis=1, keepdims=True)
    before = (
        lax.broadcasted_iota(jnp.int32, (n, n), 0) < lax.broadcasted_iota(jnp.int32, (n, n), 1)
    ).astype(jnp.float32).astype(jnp.bfloat16)
    scale = weight / total
    off = exact_dot(mass / total, before)
    t_cum = jnp.sum(t_acc, axis=1, keepdims=True)
    t_here = lane == lax.div(g_col, cols)
    t_scale = jnp.sum(jnp.where(t_here, scale, 0.0), axis=1, keepdims=True)
    t_off = jnp.sum(jnp.where(t_here, off, 0.0), axis=1, keepdims=True)
    t_val = t_cum * t_scale + t_off
    t_row = jnp.sum(jnp.where(own_lane, t_val, 0.0), axis=0, keepdims=True)
    tsend[...] = jnp.broadcast_to(t_row, tsend.shape)
    trecv[pl.ds(me, 1), :] = t_row
    sent = send.at[pl.ds(0, n - 1)]
    pltpu.make_async_copy(sent, sent, send_sem).wait()

    def tell_one(d):
        pltpu.make_async_remote_copy(
            src_ref=tsend.at[pl.ds(0, 1)],
            dst_ref=trecv.at[pl.ds(me, 1)],
            send_sem=tsend_sem,
            recv_sem=trecv_sem,
            device_id={"vp": d},
            device_id_type=MESH,
        ).start()

    def tell(step, carry):
        for j, d in enumerate(partners(me, step, steps)):
            if j < group - 1:
                tell_one(d)
            else:
                pl.when(step < steps - 1)(functools.partial(tell_one, d))
        return carry

    lax.fori_loop(0, steps, tell, 0)
    for s in range(n):
        table[:, s * cols : (s + 1) * cols] = cum[s] * scale[:, s : s + 1] + off[:, s : s + 1]
    others = trecv.at[pl.ds(0, n - 1)]
    pltpu.make_async_copy(others, others, trecv_sem).wait()
    tgt_out[...] = jnp.sum(trecv[...].reshape(n // per, per, 128), axis=1)
    pltpu.make_async_copy(others, others, tsend_sem).wait()


def store_kernel(parts, table, tgt, table_out, tgt_out, sem):
    cols = table.shape[1] // parts
    copies = [
        pltpu.make_async_copy(table.at[:, pl.ds(i * cols, cols)], table_out.at[:, pl.ds(i * cols, cols)], sem.at[i])
        for i in range(parts)
    ]
    copies.append(pltpu.make_async_copy(tgt, tgt_out, sem.at[parts]))
    for copy in copies:
        copy.start()
    for copy in copies:
        copy.wait()


def solution(mesh):
    n = mesh.shape["vp"]

    def local_step(hidden, w_local, inv_temp, target_ids):
        batch, depth = hidden.shape
        cols = w_local.shape[1]
        rows = batch // n
        group = 8
        f32 = jnp.float32
        vmem = pl.BlockSpec(memory_space=pltpu.VMEM)
        hbm = pl.BlockSpec(memory_space=pltpu.HBM)
        small = (batch // 128, 128)
        table, at_target = pl.pallas_call(
            functools.partial(exchange_kernel, n, rows, group),
            out_shape=(
                jax.ShapeDtypeStruct((rows, n * cols), f32),
                jax.ShapeDtypeStruct(small, f32),
            ),
            in_specs=[hbm] * 4,
            out_specs=(vmem, vmem),
            scratch_shapes=[
                pltpu.VMEM((depth, cols), jnp.bfloat16),
                pltpu.VMEM((SLOTS, group * rows, depth), jnp.bfloat16),
                pltpu.VMEM((n, rows, cols), f32),
                pltpu.VMEM((n, rows, cols), f32),
                pltpu.VMEM((n, rows, cols), f32),
                pltpu.VMEM(small, f32),
                pltpu.VMEM(small, jnp.int32),
                pltpu.VMEM((8, 128), f32),
                pltpu.VMEM((n, 128), f32),
                pltpu.SemaphoreType.DMA,
                pltpu.SemaphoreType.DMA((SLOTS,)),
                pltpu.SemaphoreType.DMA,
                pltpu.SemaphoreType.DMA((n // group,)),
                pltpu.SemaphoreType.DMA,
                pltpu.SemaphoreType.DMA,
                pltpu.SemaphoreType.DMA,
            ],
            compiler_params=pltpu.CompilerParams(
                collective_id=0, has_side_effects=True, vmem_limit_bytes=48 * 1024 * 1024
            ),
            name="exchange",
        )(
            hidden,
            w_local,
            pltpu.with_memory_space_constraint(inv_temp.reshape(small), pltpu.HBM),
            pltpu.with_memory_space_constraint(target_ids.reshape(small), pltpu.HBM),
        )
        parts = 4
        table, at_target = pl.pallas_call(
            functools.partial(store_kernel, parts),
            out_shape=(jax.ShapeDtypeStruct(table.shape, f32), jax.ShapeDtypeStruct(small, f32)),
            in_specs=[hbm] * 2,
            out_specs=(hbm, hbm),
            scratch_shapes=[pltpu.SemaphoreType.DMA((parts + 1,))],
            compiler_params=pltpu.CompilerParams(vmem_limit_bytes=1024 * 1024),
            name="store",
        )(table, at_target)
        return table, at_target.reshape(-1)

    return jax.shard_map(
        local_step,
        mesh=mesh,
        in_specs=(P("dp", None), P(None, "vp"), P("dp"), P("dp")),
        out_specs=(P(("dp", "vp"), None), P("dp")),
        check_vma=False,
    )
```

```python
import functools

import jax
import jax.numpy as jnp
from jax import lax
from jax.experimental import pallas as pl
from jax.experimental.pallas import tpu as pltpu
from jax.sharding import PartitionSpec as P

MESH = pl.DeviceIdType.MESH
SLOTS = 3
FINE = ((1, 4), (3, 6), (5, 2))
COARSE = (0, 2, 4, 6)
TAKE = 2
PACE = (1, 1)


def split3(x):
    hi = x.astype(jnp.bfloat16)
    rest = x - hi.astype(jnp.float32)
    mid = rest.astype(jnp.bfloat16)
    lo = (rest - mid.astype(jnp.float32)).astype(jnp.bfloat16)
    return hi, mid, lo


def exact_dot(x, ones_mask):
    hi, mid, lo = split3(x)
    dot = functools.partial(jnp.dot, preferred_element_type=jnp.float32)
    return dot(lo, ones_mask) + dot(mid, ones_mask) + dot(hi, ones_mask)


def partners(me, step, steps, sign=1):
    turned = steps - 1 - step
    coarse = [lax.rem(lax.div(turned, 1 << COARSE.index(i)), 2) if i in COARSE else 0 for i in range(7)]
    flipped = lambda bit, flip: 1 - bit if flip else bit
    core = lax.rem(me, 2)
    own = [lax.rem(lax.div(me, 2 * 4**a), 4) for a in range(3)]
    known = {}
    group = []
    for j in range(8):
        fine = [sum(i in f for t, f in enumerate(FINE) if (7 - j) >> t & 1) % 2 for i in range(7)]
        if (0, fine[0]) not in known:
            known[0, fine[0]] = lax.rem(core + flipped(coarse[0], fine[0]), 2)
        parts = [known[0, fine[0]]]
        for a in range(3):
            low, high = fine[2 * a + 1], fine[2 * a + 2]
            if (a + 1, low, high) not in known:
                offset = flipped(coarse[2 * a + 1], low) + 2 * flipped(coarse[2 * a + 2], high)
                moved = own[a] + offset if sign > 0 else own[a] + 4 - offset
                known[a + 1, low, high] = lax.rem(moved, 4) * (2 * 4**a)
            parts.append(known[a + 1, low, high])
        group.append(sum(parts))
    return group


def exchange_kernel(
    n, rows, group,
    hidden, w, temp_hbm, target_hbm,
    table, tgt_out,
    w_buf, h_buf, send, recv, cum, temp, target, tsend, trecv,
    w_sem, h_sem, send_sem, recv_sem, small_sem, tsend_sem, trecv_sem,
):
    me = lax.axis_index("vp")
    cols = w.shape[1]
    steps = n // group

    def fetch(step):
        slot = lax.rem(step, SLOTS)
        for j, d in enumerate(partners(me, step, steps)):
            pltpu.make_async_copy(
                hidden.at[pl.ds(pl.multiple_of(d * rows, rows), rows)],
                h_buf.at[slot, pl.ds(j * rows, rows)],
                h_sem.at[slot],
            ).start()

    barrier = pltpu.get_barrier_semaphore()

    def greet(step, carry):
        for j, d in enumerate(partners(me, step, steps)):
            if j < group - 1:
                pl.semaphore_signal(barrier, inc=1, device_id={"vp": d}, device_id_type=MESH)
            else:

                @pl.when(step < steps - 1)
                def _():
                    pl.semaphore_signal(barrier, inc=1, device_id={"vp": d}, device_id_type=MESH)

        return carry

    lax.fori_loop(0, steps, greet, 0)
    fetch(0)
    part = w.shape[0] // 4
    for i in range(4):
        at = pl.ds(i * part, part)
        pltpu.make_async_copy(w.at[at], w_buf.at[at], w_sem).start()
    for s in range(1, SLOTS - 1):
        fetch(s)
    pltpu.make_async_copy(temp_hbm, temp, small_sem).start()
    pltpu.make_async_copy(target_hbm, target, small_sem).start()

    def send_blocks(step, count):
        for j, d in enumerate(partners(me, step, steps)[:count]):
            pltpu.make_async_remote_copy(
                src_ref=send.at[step * group + j],
                dst_ref=recv.at[me],
                send_sem=send_sem,
                recv_sem=recv_sem.at[step],
                device_id={"vp": d},
                device_id_type=MESH,
            ).start()

    pltpu.make_async_copy(w_buf, w_buf, w_sem).wait()

    def due(step):
        return lax.div(jnp.maximum(step, 0) * PACE[0], PACE[1])

    def matmul_step(step, carry):
        slot = lax.rem(step, SLOTS)
        pltpu.make_async_copy(h_buf.at[slot], h_buf.at[slot], h_sem.at[slot]).wait()

        @pl.when(step == 1)
        def _():
            pl.semaphore_wait(barrier, n - 1)

        @pl.when(due(step) > due(step - 1))
        def _():
            send_blocks(due(step) - 1, group)

        @pl.when(step + SLOTS - 1 < steps)
        def _():
            fetch(step + SLOTS - 1)

        z = jnp.dot(h_buf[slot], w_buf[...], preferred_element_type=jnp.float32)
        send[pl.ds(step * group, group)] = z.reshape(group, rows, cols)
        return carry

    lax.fori_loop(0, steps, matmul_step, 0)
    pltpu.make_async_copy(temp, temp, small_sem).wait()
    pltpu.make_async_copy(target, target, small_sem).wait()

    per = 128 // rows
    lane = lax.broadcasted_iota(jnp.int32, (rows, 128), 1)
    row = lax.broadcasted_iota(jnp.int32, (rows, 128), 0)
    own_lane = lane == lax.rem(me, per) * rows + row
    own_at = pl.ds(lax.div(me, per), 1)
    t_col = jnp.sum(jnp.where(own_lane, temp[own_at, :], 0.0), axis=1, keepdims=True)
    g_col = jnp.sum(jnp.where(own_lane, target[own_at, :], 0), axis=1, keepdims=True)
    upto = (
        lax.broadcasted_iota(jnp.int32, (cols, cols), 0) <= lax.broadcasted_iota(jnp.int32, (cols, cols), 1)
    ).astype(jnp.float32).astype(jnp.bfloat16)
    col = lax.broadcasted_iota(jnp.int32, (rows, cols), 1)

    for step in range((steps - 1) * PACE[0] // PACE[1], steps):
        send_blocks(step, group if step < steps - 1 else group - 1)
    recv[me] = send[n - 1]

    def arrived(step, count):
        whole = recv.at[pl.ds(0, count)]
        pltpu.make_async_copy(whole, whole, recv_sem.at[step]).wait()

    def take(turn, carry):
        m_all, s_all, t_acc = carry
        first = turn * TAKE
        for i in range(TAKE - 1):
            arrived(first + i, group)
        pl.when(turn < steps // TAKE - 1)(functools.partial(arrived, first + TAKE - 1, group))
        pl.when(turn == steps // TAKE - 1)(functools.partial(arrived, first + TAKE - 1, group - 1))
        source = [d for i in range(TAKE) for d in partners(me, first + i, steps, -1)]
        z = [recv[s] * t_col for s in source]
        m = [jnp.max(v, axis=1, keepdims=True) for v in z]
        e = jnp.concatenate([jnp.exp(v - u) for v, u in zip(z, m)], axis=0)
        c = exact_dot(e, upto)
        for j, s in enumerate(source):
            c_j = c[j * rows : (j + 1) * rows]
            cum[s] = c_j
            here = lane == s
            m_all = jnp.where(here, m[j], m_all)
            s_all = jnp.where(here, c_j[:, cols - 1 :], s_all)
            t_acc = t_acc + jnp.where(col == g_col - s * cols, c_j, 0.0)
        return m_all, s_all, t_acc

    zero = jnp.zeros((rows, 128), jnp.float32)
    m_all, s_all, t_acc = lax.fori_loop(0, steps // TAKE, take, (zero, zero, jnp.zeros((rows, cols), jnp.float32)))

    top = jnp.max(m_all, axis=1, keepdims=True)
    weight = jnp.exp(m_all - top)
    mass = s_all * weight
    total = jnp.sum(mass, axis=1, keepdims=True)
    scale = weight / total
    share = mass / total
    t_cum = jnp.sum(t_acc, axis=1, keepdims=True)
    t_here = lane == lax.div(g_col, cols)
    t_scale = jnp.sum(jnp.where(t_here, scale, 0.0), axis=1, keepdims=True)
    t_off = jnp.sum(jnp.where(lane < lax.div(g_col, cols), share, 0.0), axis=1, keepdims=True)
    t_val = t_cum * t_scale + t_off
    t_row = jnp.sum(jnp.where(own_lane, t_val, 0.0), axis=0, keepdims=True)
    tsend[...] = jnp.broadcast_to(t_row, tsend.shape)
    trecv[pl.ds(me, 1), :] = t_row
    sent = send.at[pl.ds(0, n - 1)]
    pltpu.make_async_copy(sent, sent, send_sem).wait()

    def tell_one(d):
        pltpu.make_async_remote_copy(
            src_ref=tsend.at[pl.ds(0, 1)],
            dst_ref=trecv.at[pl.ds(me, 1)],
            send_sem=tsend_sem,
            recv_sem=trecv_sem,
            device_id={"vp": d},
            device_id_type=MESH,
        ).start()

    def tell(step, carry):
        for j, d in enumerate(partners(me, step, steps)):
            if j < group - 1:
                tell_one(d)
            else:
                pl.when(step < steps - 1)(functools.partial(tell_one, d))
        return carry

    lax.fori_loop(0, steps, tell, 0)
    before = (
        lax.broadcasted_iota(jnp.int32, (n, n), 0) < lax.broadcasted_iota(jnp.int32, (n, n), 1)
    ).astype(jnp.float32).astype(jnp.bfloat16)
    off = exact_dot(share, before)
    for s in range(n):
        table[:, s * cols : (s + 1) * cols] = cum[s] * scale[:, s : s + 1] + off[:, s : s + 1]
    others = trecv.at[pl.ds(0, n - 1)]
    pltpu.make_async_copy(others, others, trecv_sem).wait()
    tgt_out[...] = jnp.sum(trecv[...].reshape(n // per, per, 128), axis=1)
    pltpu.make_async_copy(others, others, tsend_sem).wait()


def store_kernel(parts, table, tgt, table_out, tgt_out, sem):
    cols = table.shape[1] // parts
    copies = [
        pltpu.make_async_copy(table.at[:, pl.ds(i * cols, cols)], table_out.at[:, pl.ds(i * cols, cols)], sem.at[i])
        for i in range(parts)
    ]
    copies.append(pltpu.make_async_copy(tgt, tgt_out, sem.at[parts]))
    for copy in copies:
        copy.start()
    for copy in copies:
        copy.wait()


def solution(mesh):
    n = mesh.shape["vp"]

    def local_step(hidden, w_local, inv_temp, target_ids):
        batch, depth = hidden.shape
        cols = w_local.shape[1]
        rows = batch // n
        group = 8
        f32 = jnp.float32
        vmem = pl.BlockSpec(memory_space=pltpu.VMEM)
        hbm = pl.BlockSpec(memory_space=pltpu.HBM)
        small = (batch // 128, 128)
        table, at_target = pl.pallas_call(
            functools.partial(exchange_kernel, n, rows, group),
            out_shape=(
                jax.ShapeDtypeStruct((rows, n * cols), f32),
                jax.ShapeDtypeStruct(small, f32),
            ),
            in_specs=[hbm] * 4,
            out_specs=(vmem, vmem),
            scratch_shapes=[
                pltpu.VMEM((depth, cols), jnp.bfloat16),
                pltpu.VMEM((SLOTS, group * rows, depth), jnp.bfloat16),
                pltpu.VMEM((n, rows, cols), f32),
                pltpu.VMEM((n, rows, cols), f32),
                pltpu.VMEM((n, rows, cols), f32),
                pltpu.VMEM(small, f32),
                pltpu.VMEM(small, jnp.int32),
                pltpu.VMEM((8, 128), f32),
                pltpu.VMEM((n, 128), f32),
                pltpu.SemaphoreType.DMA,
                pltpu.SemaphoreType.DMA((SLOTS,)),
                pltpu.SemaphoreType.DMA,
                pltpu.SemaphoreType.DMA((n // group,)),
                pltpu.SemaphoreType.DMA,
                pltpu.SemaphoreType.DMA,
                pltpu.SemaphoreType.DMA,
            ],
            compiler_params=pltpu.CompilerParams(
                collective_id=0, has_side_effects=True, vmem_limit_bytes=48 * 1024 * 1024
            ),
            name="exchange",
        )(
            hidden,
            w_local,
            pltpu.with_memory_space_constraint(inv_temp.reshape(small), pltpu.HBM),
            pltpu.with_memory_space_constraint(target_ids.reshape(small), pltpu.HBM),
        )
        parts = 4
        table, at_target = pl.pallas_call(
            functools.partial(store_kernel, parts),
            out_shape=(jax.ShapeDtypeStruct(table.shape, f32), jax.ShapeDtypeStruct(small, f32)),
            in_specs=[hbm] * 2,
            out_specs=(hbm, hbm),
            scratch_shapes=[pltpu.SemaphoreType.DMA((parts + 1,))],
            compiler_params=pltpu.CompilerParams(vmem_limit_bytes=1024 * 1024),
            name="store",
        )(table, at_target)
        return table, at_target.reshape(-1)

    return jax.shard_map(
        local_step,
        mesh=mesh,
        in_specs=(P("dp", None), P(None, "vp"), P("dp"), P("dp")),
        out_specs=(P(("dp", "vp"), None), P("dp")),
        check_vma=False,
    )
```

```python
import functools

import jax
import jax.numpy as jnp
from jax import lax
from jax.experimental import pallas as pl
from jax.experimental.pallas import tpu as pltpu
from jax.sharding import PartitionSpec as P

MESH = pl.DeviceIdType.MESH
SLOTS = 3
FINE = ((1, 6), (3, 2), (5, 4))
COARSE = (6, 4, 2, 0)
TAKE = 2
PACE = (1, 1)


def split3(x):
    hi = x.astype(jnp.bfloat16)
    rest = x - hi.astype(jnp.float32)
    mid = rest.astype(jnp.bfloat16)
    lo = (rest - mid.astype(jnp.float32)).astype(jnp.bfloat16)
    return hi, mid, lo


def exact_dot(x, ones_mask):
    three = jnp.concatenate(split3(x)[::-1], axis=1)
    return jnp.dot(three, jnp.concatenate([ones_mask] * 3, axis=0), preferred_element_type=jnp.float32)


def partners(me, step, steps, sign=1):
    turned = steps - 1 - step
    coarse = [lax.rem(lax.div(turned, 1 << COARSE.index(i)), 2) if i in COARSE else 0 for i in range(7)]
    flipped = lambda bit, flip: 1 - bit if flip else bit
    core = lax.rem(me, 2)
    own = [lax.rem(lax.div(me, 2 * 4**a), 4) for a in range(3)]
    known = {}
    group = []
    for j in range(8):
        fine = [sum(i in f for t, f in enumerate(FINE) if (7 - j) >> t & 1) % 2 for i in range(7)]
        if (0, fine[0]) not in known:
            known[0, fine[0]] = lax.rem(core + flipped(coarse[0], fine[0]), 2)
        parts = [known[0, fine[0]]]
        for a in range(3):
            low, high = fine[2 * a + 1], fine[2 * a + 2]
            if (a + 1, low, high) not in known:
                offset = flipped(coarse[2 * a + 1], low) + 2 * flipped(coarse[2 * a + 2], high)
                moved = own[a] + offset if sign > 0 else own[a] + 4 - offset
                known[a + 1, low, high] = lax.rem(moved, 4) * (2 * 4**a)
            parts.append(known[a + 1, low, high])
        group.append(sum(parts))
    return group


def exchange_kernel(
    n, rows, group,
    hidden, w, temp_hbm, target_hbm,
    table, tgt_out,
    w_buf, h_buf, send, recv, cum, temp, target, tsend, trecv,
    w_sem, h_sem, send_sem, recv_sem, small_sem, tsend_sem, trecv_sem,
):
    me = lax.axis_index("vp")
    cols = w.shape[1]
    steps = n // group

    def fetch(step):
        slot = lax.rem(step, SLOTS)
        for j, d in enumerate(partners(me, step, steps)):
            pltpu.make_async_copy(
                hidden.at[pl.ds(pl.multiple_of(d * rows, rows), rows)],
                h_buf.at[slot, pl.ds(j * rows, rows)],
                h_sem.at[slot],
            ).start()

    fetch(0)
    part = w.shape[0] // 4
    for i in range(4):
        at = pl.ds(i * part, part)
        pltpu.make_async_copy(w.at[at], w_buf.at[at], w_sem).start()
    barrier = pltpu.get_barrier_semaphore()

    def greet(step, carry):
        for j, d in enumerate(partners(me, step, steps)):
            if j < group - 1:
                pl.semaphore_signal(barrier, inc=1, device_id={"vp": d}, device_id_type=MESH)
            else:

                @pl.when(step < steps - 1)
                def _():
                    pl.semaphore_signal(barrier, inc=1, device_id={"vp": d}, device_id_type=MESH)

        return carry

    lax.fori_loop(0, steps, greet, 0)
    for s in range(1, SLOTS - 1):
        fetch(s)
    pltpu.make_async_copy(temp_hbm, temp, small_sem).start()
    pltpu.make_async_copy(target_hbm, target, small_sem).start()

    def send_blocks(step, count):
        for j, d in enumerate(partners(me, step, steps)[:count]):
            pltpu.make_async_remote_copy(
                src_ref=send.at[step * group + j],
                dst_ref=recv.at[me],
                send_sem=send_sem,
                recv_sem=recv_sem.at[step],
                device_id={"vp": d},
                device_id_type=MESH,
            ).start()

    pltpu.make_async_copy(w_buf, w_buf, w_sem).wait()

    def due(step):
        return lax.div(jnp.maximum(step, 0) * PACE[0], PACE[1])

    def matmul_step(step, carry):
        slot = lax.rem(step, SLOTS)
        pltpu.make_async_copy(h_buf.at[slot], h_buf.at[slot], h_sem.at[slot]).wait()

        @pl.when(step == 1)
        def _():
            pl.semaphore_wait(barrier, n - 1)

        @pl.when(due(step) > due(step - 1))
        def _():
            send_blocks(due(step) - 1, group)

        @pl.when(step + SLOTS - 1 < steps)
        def _():
            fetch(step + SLOTS - 1)

        z = jnp.dot(h_buf[slot], w_buf[...], preferred_element_type=jnp.float32)
        send[pl.ds(step * group, group)] = z.reshape(group, rows, cols)
        return carry

    lax.fori_loop(0, steps, matmul_step, 0)
    pltpu.make_async_copy(temp, temp, small_sem).wait()
    pltpu.make_async_copy(target, target, small_sem).wait()

    per = 128 // rows
    lane = lax.broadcasted_iota(jnp.int32, (rows, 128), 1)
    row = lax.broadcasted_iota(jnp.int32, (rows, 128), 0)
    own_lane = lane == lax.rem(me, per) * rows + row
    own_at = pl.ds(lax.div(me, per), 1)
    t_col = jnp.sum(jnp.where(own_lane, temp[own_at, :], 0.0), axis=1, keepdims=True)
    g_col = jnp.sum(jnp.where(own_lane, target[own_at, :], 0), axis=1, keepdims=True)
    upto = (
        lax.broadcasted_iota(jnp.int32, (cols, cols), 0) <= lax.broadcasted_iota(jnp.int32, (cols, cols), 1)
    ).astype(jnp.float32).astype(jnp.bfloat16)
    col = lax.broadcasted_iota(jnp.int32, (rows, cols), 1)

    for step in range((steps - 1) * PACE[0] // PACE[1], steps):
        send_blocks(step, group if step < steps - 1 else group - 1)
    recv[me] = send[n - 1]

    def arrived(step, count):
        whole = recv.at[pl.ds(0, count)]
        pltpu.make_async_copy(whole, whole, recv_sem.at[step]).wait()

    def take(turn, carry):
        m_all, s_all, t_acc = carry
        first = turn * TAKE
        for i in range(TAKE - 1):
            arrived(first + i, group)
        pl.when(turn < steps // TAKE - 1)(functools.partial(arrived, first + TAKE - 1, group))
        pl.when(turn == steps // TAKE - 1)(functools.partial(arrived, first + TAKE - 1, group - 1))
        source = [d for i in range(TAKE) for d in partners(me, first + i, steps, -1)]
        z = [recv[s] * t_col for s in source]
        m = [jnp.max(v, axis=1, keepdims=True) for v in z]
        e = jnp.concatenate([jnp.exp(v - u) for v, u in zip(z, m)], axis=0)
        c = exact_dot(e, upto)
        for j, s in enumerate(source):
            c_j = c[j * rows : (j + 1) * rows]
            cum[s] = c_j
            here = lane == s
            m_all = jnp.where(here, m[j], m_all)
            s_all = jnp.where(here, c_j[:, cols - 1 :], s_all)
            t_acc = t_acc + jnp.where(col == g_col - s * cols, c_j, 0.0)
        return m_all, s_all, t_acc

    zero = jnp.zeros((rows, 128), jnp.float32)
    m_all, s_all, t_acc = lax.fori_loop(0, steps // TAKE, take, (zero, zero, jnp.zeros((rows, cols), jnp.float32)))

    top = jnp.max(m_all, axis=1, keepdims=True)
    weight = jnp.exp(m_all - top)
    mass = s_all * weight
    total = jnp.sum(mass, axis=1, keepdims=True)
    scale = weight / total
    share = mass / total
    t_cum = jnp.sum(t_acc, axis=1, keepdims=True)
    t_here = lane == lax.div(g_col, cols)
    t_scale = jnp.sum(jnp.where(t_here, scale, 0.0), axis=1, keepdims=True)
    t_off = jnp.sum(jnp.where(lane < lax.div(g_col, cols), share, 0.0), axis=1, keepdims=True)
    t_val = t_cum * t_scale + t_off
    t_row = jnp.sum(jnp.where(own_lane, t_val, 0.0), axis=0, keepdims=True)
    tsend[...] = jnp.broadcast_to(t_row, tsend.shape)
    trecv[pl.ds(me, 1), :] = t_row
    sent = send.at[pl.ds(0, n - 1)]
    pltpu.make_async_copy(sent, sent, send_sem).wait()

    def tell_one(d):
        pltpu.make_async_remote_copy(
            src_ref=tsend.at[pl.ds(0, 1)],
            dst_ref=trecv.at[pl.ds(me, 1)],
            send_sem=tsend_sem,
            recv_sem=trecv_sem,
            device_id={"vp": d},
            device_id_type=MESH,
        ).start()

    def tell(step, carry):
        for j, d in enumerate(partners(me, step, steps)):
            if j < group - 1:
                tell_one(d)
            else:
                pl.when(step < steps - 1)(functools.partial(tell_one, d))
        return carry

    lax.fori_loop(0, steps, tell, 0)
    before = (
        lax.broadcasted_iota(jnp.int32, (n, n), 0) < lax.broadcasted_iota(jnp.int32, (n, n), 1)
    ).astype(jnp.float32).astype(jnp.bfloat16)
    off = exact_dot(share, before)
    for s in range(n):
        table[:, s * cols : (s + 1) * cols] = cum[s] * scale[:, s : s + 1] + off[:, s : s + 1]
    others = trecv.at[pl.ds(0, n - 1)]
    pltpu.make_async_copy(others, others, trecv_sem).wait()
    tgt_out[...] = jnp.sum(trecv[...].reshape(n // per, per, 128), axis=1)
    pltpu.make_async_copy(others, others, tsend_sem).wait()


def store_kernel(parts, table, tgt, table_out, tgt_out, sem):
    cols = table.shape[1] // parts
    copies = [
        pltpu.make_async_copy(table.at[:, pl.ds(i * cols, cols)], table_out.at[:, pl.ds(i * cols, cols)], sem.at[i])
        for i in range(parts)
    ]
    copies.append(pltpu.make_async_copy(tgt, tgt_out, sem.at[parts]))
    for copy in copies:
        copy.start()
    for copy in copies:
        copy.wait()


def solution(mesh):
    n = mesh.shape["vp"]

    def local_step(hidden, w_local, inv_temp, target_ids):
        batch, depth = hidden.shape
        cols = w_local.shape[1]
        rows = batch // n
        group = 8
        f32 = jnp.float32
        vmem = pl.BlockSpec(memory_space=pltpu.VMEM)
        hbm = pl.BlockSpec(memory_space=pltpu.HBM)
        small = (batch // 128, 128)
        table, at_target = pl.pallas_call(
            functools.partial(exchange_kernel, n, rows, group),
            out_shape=(
                jax.ShapeDtypeStruct((rows, n * cols), f32),
                jax.ShapeDtypeStruct(small, f32),
            ),
            in_specs=[hbm] * 4,
            out_specs=(vmem, vmem),
            scratch_shapes=[
                pltpu.VMEM((depth, cols), jnp.bfloat16),
                pltpu.VMEM((SLOTS, group * rows, depth), jnp.bfloat16),
                pltpu.VMEM((n, rows, cols), f32),
                pltpu.VMEM((n, rows, cols), f32),
                pltpu.VMEM((n, rows, cols), f32),
                pltpu.VMEM(small, f32),
                pltpu.VMEM(small, jnp.int32),
                pltpu.VMEM((8, 128), f32),
                pltpu.VMEM((n, 128), f32),
                pltpu.SemaphoreType.DMA,
                pltpu.SemaphoreType.DMA((SLOTS,)),
                pltpu.SemaphoreType.DMA,
                pltpu.SemaphoreType.DMA((n // group,)),
                pltpu.SemaphoreType.DMA,
                pltpu.SemaphoreType.DMA,
                pltpu.SemaphoreType.DMA,
            ],
            compiler_params=pltpu.CompilerParams(
                collective_id=0, has_side_effects=True, vmem_limit_bytes=48 * 1024 * 1024
            ),
            name="exchange",
        )(
            hidden,
            w_local,
            pltpu.with_memory_space_constraint(inv_temp.reshape(small), pltpu.HBM),
            pltpu.with_memory_space_constraint(target_ids.reshape(small), pltpu.HBM),
        )
        parts = 4
        table, at_target = pl.pallas_call(
            functools.partial(store_kernel, parts),
            out_shape=(jax.ShapeDtypeStruct(table.shape, f32), jax.ShapeDtypeStruct(small, f32)),
            in_specs=[hbm] * 2,
            out_specs=(hbm, hbm),
            scratch_shapes=[pltpu.SemaphoreType.DMA((parts + 1,))],
            compiler_params=pltpu.CompilerParams(vmem_limit_bytes=1024 * 1024),
            name="store",
        )(table, at_target)
        return table, at_target.reshape(-1)

    return jax.shard_map(
        local_step,
        mesh=mesh,
        in_specs=(P("dp", None), P(None, "vp"), P("dp"), P("dp")),
        out_specs=(P(("dp", "vp"), None), P("dp")),
        check_vma=False,
    )
```

```python
import functools

import jax
import jax.numpy as jnp
from jax import lax
from jax.experimental import pallas as pl
from jax.experimental.pallas import tpu as pltpu
from jax.sharding import PartitionSpec as P

MESH = pl.DeviceIdType.MESH
SLOTS = 3
FINE = ((1, 2), (3, 4), (5, 6))
COARSE = (6, 4, 2, 0)
TAKE = 2
PACE = (1, 1)


def split3(x):
    hi = x.astype(jnp.bfloat16)
    rest = x - hi.astype(jnp.float32)
    mid = rest.astype(jnp.bfloat16)
    lo = (rest - mid.astype(jnp.float32)).astype(jnp.bfloat16)
    return hi, mid, lo


def exact_dot(x, ones_mask):
    three = jnp.concatenate(split3(x)[::-1], axis=1)
    return jnp.dot(three, jnp.concatenate([ones_mask] * 3, axis=0), preferred_element_type=jnp.float32)


def partners(me, step, steps, sign=1):
    turned = steps - 1 - step
    coarse = [lax.rem(lax.div(turned, 1 << COARSE.index(i)), 2) if i in COARSE else 0 for i in range(7)]
    flipped = lambda bit, flip: 1 - bit if flip else bit
    core = lax.rem(me, 2)
    own = [lax.rem(lax.div(me, 2 * 4**a), 4) for a in range(3)]
    known = {}
    group = []
    for j in range(8):
        fine = [sum(i in f for t, f in enumerate(FINE) if (7 - j) >> t & 1) % 2 for i in range(7)]
        if (0, fine[0]) not in known:
            known[0, fine[0]] = lax.rem(core + flipped(coarse[0], fine[0]), 2)
        parts = [known[0, fine[0]]]
        for a in range(3):
            low, high = fine[2 * a + 1], fine[2 * a + 2]
            if (a + 1, low, high) not in known:
                offset = flipped(coarse[2 * a + 1], low) + 2 * flipped(coarse[2 * a + 2], high)
                moved = own[a] + offset if sign > 0 else own[a] + 4 - offset
                known[a + 1, low, high] = lax.rem(moved, 4) * (2 * 4**a)
            parts.append(known[a + 1, low, high])
        group.append(sum(parts))
    return group


def exchange_kernel(
    n, rows, group,
    hidden, w, temp_hbm, target_hbm,
    table, tgt_out,
    w_buf, h_buf, send, recv, cum, temp, target, tsend, trecv,
    w_sem, h_sem, send_sem, recv_sem, small_sem, tsend_sem, trecv_sem,
):
    me = lax.axis_index("vp")
    cols = w.shape[1]
    steps = n // group

    def fetch(step):
        slot = lax.rem(step, SLOTS)
        for j, d in enumerate(partners(me, step, steps)):
            pltpu.make_async_copy(
                hidden.at[pl.ds(pl.multiple_of(d * rows, rows), rows)],
                h_buf.at[slot, pl.ds(j * rows, rows)],
                h_sem.at[slot],
            ).start()

    fetch(0)
    part = w.shape[0] // 4
    for i in range(4):
        at = pl.ds(i * part, part)
        pltpu.make_async_copy(w.at[at], w_buf.at[at], w_sem).start()
    barrier = pltpu.get_barrier_semaphore()

    def greet(step, carry):
        for j, d in enumerate(partners(me, step, steps)):
            if j < group - 1:
                pl.semaphore_signal(barrier, inc=1, device_id={"vp": d}, device_id_type=MESH)
            else:

                @pl.when(step < steps - 1)
                def _():
                    pl.semaphore_signal(barrier, inc=1, device_id={"vp": d}, device_id_type=MESH)

        return carry

    lax.fori_loop(0, steps, greet, 0)
    for s in range(1, SLOTS - 1):
        fetch(s)
    pltpu.make_async_copy(temp_hbm, temp, small_sem).start()
    pltpu.make_async_copy(target_hbm, target, small_sem).start()

    def send_blocks(step, count):
        for j, d in enumerate(partners(me, step, steps)[:count]):
            pltpu.make_async_remote_copy(
                src_ref=send.at[step * group + j],
                dst_ref=recv.at[me],
                send_sem=send_sem,
                recv_sem=recv_sem.at[step],
                device_id={"vp": d},
                device_id_type=MESH,
            ).start()

    pltpu.make_async_copy(w_buf, w_buf, w_sem).wait()

    def due(step):
        return lax.div(jnp.maximum(step, 0) * PACE[0], PACE[1])

    def matmul_step(step, carry):
        slot = lax.rem(step, SLOTS)
        pltpu.make_async_copy(h_buf.at[slot], h_buf.at[slot], h_sem.at[slot]).wait()

        @pl.when(step == 1)
        def _():
            pl.semaphore_wait(barrier, n - 1)

        @pl.when(due(step) > due(step - 1))
        def _():
            send_blocks(due(step) - 1, group)

        @pl.when(step + SLOTS - 1 < steps)
        def _():
            fetch(step + SLOTS - 1)

        z = jnp.dot(h_buf[slot], w_buf[...], preferred_element_type=jnp.float32)
        send[pl.ds(step * group, group)] = z.reshape(group, rows, cols)
        return carry

    lax.fori_loop(0, steps, matmul_step, 0)
    pltpu.make_async_copy(temp, temp, small_sem).wait()
    pltpu.make_async_copy(target, target, small_sem).wait()

    per = 128 // rows
    lane = lax.broadcasted_iota(jnp.int32, (rows, 128), 1)
    row = lax.broadcasted_iota(jnp.int32, (rows, 128), 0)
    own_lane = lane == lax.rem(me, per) * rows + row
    own_at = pl.ds(lax.div(me, per), 1)
    t_col = jnp.sum(jnp.where(own_lane, temp[own_at, :], 0.0), axis=1, keepdims=True)
    g_col = jnp.sum(jnp.where(own_lane, target[own_at, :], 0), axis=1, keepdims=True)
    upto = (
        lax.broadcasted_iota(jnp.int32, (cols, cols), 0) <= lax.broadcasted_iota(jnp.int32, (cols, cols), 1)
    ).astype(jnp.float32).astype(jnp.bfloat16)
    col = lax.broadcasted_iota(jnp.int32, (rows, cols), 1)

    for step in range((steps - 1) * PACE[0] // PACE[1], steps):
        send_blocks(step, group if step < steps - 1 else group - 1)
    recv[me] = send[n - 1]

    def arrived(step, count):
        whole = recv.at[pl.ds(0, count)]
        pltpu.make_async_copy(whole, whole, recv_sem.at[step]).wait()

    def take(turn, carry):
        m_all, s_all, t_acc = carry
        first = turn * TAKE
        for i in range(TAKE - 1):
            arrived(first + i, group)
        pl.when(turn < steps // TAKE - 1)(functools.partial(arrived, first + TAKE - 1, group))
        pl.when(turn == steps // TAKE - 1)(functools.partial(arrived, first + TAKE - 1, group - 1))
        source = [d for i in range(TAKE) for d in partners(me, first + i, steps, -1)]
        z = [recv[s] * t_col for s in source]
        m = [jnp.max(v, axis=1, keepdims=True) for v in z]
        e = jnp.concatenate([jnp.exp(v - u) for v, u in zip(z, m)], axis=0)
        c = exact_dot(e, upto)
        for j, s in enumerate(source):
            c_j = c[j * rows : (j + 1) * rows]
            cum[s] = c_j
            here = lane == s
            m_all = jnp.where(here, m[j], m_all)
            s_all = jnp.where(here, c_j[:, cols - 1 :], s_all)
            t_acc = t_acc + jnp.where(col == g_col - s * cols, c_j, 0.0)
        return m_all, s_all, t_acc

    zero = jnp.zeros((rows, 128), jnp.float32)
    m_all, s_all, t_acc = lax.fori_loop(0, steps // TAKE, take, (zero, zero, jnp.zeros((rows, cols), jnp.float32)))

    top = jnp.max(m_all, axis=1, keepdims=True)
    weight = jnp.exp(m_all - top)
    mass = s_all * weight
    total = jnp.sum(mass, axis=1, keepdims=True)
    scale = weight / total
    share = mass / total
    t_cum = jnp.sum(t_acc, axis=1, keepdims=True)
    t_here = lane == lax.div(g_col, cols)
    t_scale = jnp.sum(jnp.where(t_here, scale, 0.0), axis=1, keepdims=True)
    t_off = jnp.sum(jnp.where(lane < lax.div(g_col, cols), share, 0.0), axis=1, keepdims=True)
    t_val = t_cum * t_scale + t_off
    t_row = jnp.sum(jnp.where(own_lane, t_val, 0.0), axis=0, keepdims=True)
    tsend[...] = jnp.broadcast_to(t_row, tsend.shape)
    trecv[pl.ds(me, 1), :] = t_row
    sent = send.at[pl.ds(0, n - 1)]
    pltpu.make_async_copy(sent, sent, send_sem).wait()

    def tell_one(d):
        pltpu.make_async_remote_copy(
            src_ref=tsend.at[pl.ds(0, 1)],
            dst_ref=trecv.at[pl.ds(me, 1)],
            send_sem=tsend_sem,
            recv_sem=trecv_sem,
            device_id={"vp": d},
            device_id_type=MESH,
        ).start()

    def tell(step, carry):
        for j, d in enumerate(partners(me, step, steps)):
            if j < group - 1:
                tell_one(d)
            else:
                pl.when(step < steps - 1)(functools.partial(tell_one, d))
        return carry

    lax.fori_loop(0, steps, tell, 0)
    before = (
        lax.broadcasted_iota(jnp.int32, (n, n), 0) < lax.broadcasted_iota(jnp.int32, (n, n), 1)
    ).astype(jnp.float32).astype(jnp.bfloat16)
    off = exact_dot(share, before)
    for s in range(n):
        table[:, s * cols : (s + 1) * cols] = cum[s] * scale[:, s : s + 1] + off[:, s : s + 1]
    others = trecv.at[pl.ds(0, n - 1)]
    pltpu.make_async_copy(others, others, trecv_sem).wait()
    tgt_out[...] = jnp.sum(trecv[...].reshape(n // per, per, 128), axis=1)
    pltpu.make_async_copy(others, others, tsend_sem).wait()


def store_kernel(parts, table, tgt, table_out, tgt_out, sem):
    cols = table.shape[1] // parts
    copies = [
        pltpu.make_async_copy(table.at[:, pl.ds(i * cols, cols)], table_out.at[:, pl.ds(i * cols, cols)], sem.at[i])
        for i in range(parts)
    ]
    copies.append(pltpu.make_async_copy(tgt, tgt_out, sem.at[parts]))
    for copy in copies:
        copy.start()
    for copy in copies:
        copy.wait()


def solution(mesh):
    n = mesh.shape["vp"]

    def local_step(hidden, w_local, inv_temp, target_ids):
        batch, depth = hidden.shape
        cols = w_local.shape[1]
        rows = batch // n
        group = 8
        f32 = jnp.float32
        vmem = pl.BlockSpec(memory_space=pltpu.VMEM)
        hbm = pl.BlockSpec(memory_space=pltpu.HBM)
        small = (batch // 128, 128)
        table, at_target = pl.pallas_call(
            functools.partial(exchange_kernel, n, rows, group),
            out_shape=(
                jax.ShapeDtypeStruct((rows, n * cols), f32),
                jax.ShapeDtypeStruct(small, f32),
            ),
            in_specs=[hbm] * 4,
            out_specs=(vmem, vmem),
            scratch_shapes=[
                pltpu.VMEM((depth, cols), jnp.bfloat16),
                pltpu.VMEM((SLOTS, group * rows, depth), jnp.bfloat16),
                pltpu.VMEM((n, rows, cols), f32),
                pltpu.VMEM((n, rows, cols), f32),
                pltpu.VMEM((n, rows, cols), f32),
                pltpu.VMEM(small, f32),
                pltpu.VMEM(small, jnp.int32),
                pltpu.VMEM((8, 128), f32),
                pltpu.VMEM((n, 128), f32),
                pltpu.SemaphoreType.DMA,
                pltpu.SemaphoreType.DMA((SLOTS,)),
                pltpu.SemaphoreType.DMA,
                pltpu.SemaphoreType.DMA((n // group,)),
                pltpu.SemaphoreType.DMA,
                pltpu.SemaphoreType.DMA,
                pltpu.SemaphoreType.DMA,
            ],
            compiler_params=pltpu.CompilerParams(
                collective_id=0, has_side_effects=True, vmem_limit_bytes=48 * 1024 * 1024
            ),
            name="exchange",
        )(
            hidden,
            w_local,
            pltpu.with_memory_space_constraint(inv_temp.reshape(small), pltpu.HBM),
            pltpu.with_memory_space_constraint(target_ids.reshape(small), pltpu.HBM),
        )
        parts = 4
        table, at_target = pl.pallas_call(
            functools.partial(store_kernel, parts),
            out_shape=(jax.ShapeDtypeStruct(table.shape, f32), jax.ShapeDtypeStruct(small, f32)),
            in_specs=[hbm] * 2,
            out_specs=(hbm, hbm),
            scratch_shapes=[pltpu.SemaphoreType.DMA((parts + 1,))],
            compiler_params=pltpu.CompilerParams(vmem_limit_bytes=1024 * 1024),
            name="store",
        )(table, at_target)
        return table, at_target.reshape(-1)

    return jax.shard_map(
        local_step,
        mesh=mesh,
        in_specs=(P("dp", None), P(None, "vp"), P("dp"), P("dp")),
        out_specs=(P(("dp", "vp"), None), P("dp")),
        check_vma=False,
    )
```
